32 devices in a mesh: dp: 16 (over z, x, core), tensor: 2 (over y).
Axes of the slice: x: 2, y: 2, z: 4, core: 2. Of those that a mesh axis runs over, the one named last changes fastest.
Arguments:
- tokens: bfloat16 [16384, 1536], P(('dp', 'tensor')), may hold values from -6 to 6
- seg_ids: int32 [16384], P('dp'), may hold values from 0 to 4, as said below
- gain_attn: bfloat16 [1536], P('dp'), may hold values from 0.5 to 1.5
- w_query: bfloat16 [1536, 1536], P('dp', 'tensor'), may hold values from -0.21875 to 0.21875
- w_key: bfloat16 [1536, 1536], P('dp', 'tensor'), may hold values from -0.21875 to 0.21875
- w_value: bfloat16 [1536, 1536], P('dp', 'tensor'), may hold values from -0.15625 to 0.15625
- w_outgate: bfloat16 [1536, 1536], P('dp', 'tensor'), may hold values from -0.15625 to 0.15625
- w_forget: bfloat16 [1536, 24], P('dp', 'tensor'), may hold values from -0.15625 to 0.15625
- forget_bias: bfloat16 [24], P('tensor'), may hold values from 1 to 7
- w_out: bfloat16 [1536, 1536], P('dp', 'tensor'), may hold values from -0.875 to 0.875
- gain_mlp: bfloat16 [1536], P('dp'), may hold values from 0.5 to 1.5
- w_gate: bfloat16 [1536, 4096], P('dp', 'tensor'), may hold values from -0.15625 to 0.15625
- w_up: bfloat16 [1536, 4096], P('dp', 'tensor'), may hold values from -0.15625 to 0.15625
- w_down: bfloat16 [1536, 4096], P('dp', 'tensor'), may hold values from -0.09375 to 0.09375
- grad_output: bfloat16 [16384, 1536], P(('dp', 'tensor')), may hold values from -6 to 6
Outputs:
- output: bfloat16 [16384, 1536], P(('dp', 'tensor'))
- grad_tokens: bfloat16 [16384, 1536], P(('dp', 'tensor'))
- grad_gain_attn: float32 [1536], P('dp')
- grad_w_query: float32 [1536, 1536], P('dp', 'tensor')
- grad_w_key: float32 [1536, 1536], P('dp', 'tensor')
- grad_w_value: float32 [1536, 1536], P('dp', 'tensor')
- grad_w_outgate: float32 [1536, 1536], P('dp', 'tensor')
- grad_w_forget: float32 [1536, 24], P('dp', 'tensor')
- grad_forget_bias: float32 [24], P('tensor')
- grad_w_out: float32 [1536, 1536], P('dp', 'tensor')
- grad_gain_mlp: float32 [1536], P('dp')
- grad_w_gate: float32 [1536, 4096], P('dp', 'tensor')
- grad_w_up: float32 [1536, 4096], P('dp', 'tensor')
- grad_w_down: float32 [1536, 4096], P('dp', 'tensor')
The draws below stay inside these ranges and needn't reach their ends.
Inputs may be any that keep to these rules, and one draw needn't show every extreme that they name: `seg_ids`: each sequence of 1024 rows holds 4 documents numbered 1 to 4 in order, each of one or more tokens, followed by 1 to 128 padding tokens with id 0.
All inputs are finite; a program needn't handle non-finite values.
Results may differ from the reference program's by a relative error of at most 0.015.
Values may be sent and summed in bfloat16 or wider, within the bound.
A program may use at most 320 MiB of HBM per device.

```python
import jax
import jax.numpy as jnp
from jax import lax

D = 1536
H = 24
HS = 64
FF = 4096
LEN = 1024
DOCS = 4
TOKENS = 16384


def draw_seg_ids(key, part):
    seq_count = TOKENS // LEN
    cut_span = LEN - LEN // 8 - 2
    seq_keys = jax.random.split(key, seq_count)

    def draw_single(seq_key):
        key_cuts, key_pad = jax.random.split(seq_key)
        shuffled = jax.random.permutation(key_cuts, cut_span)
        cut_flags = (shuffled < DOCS - 1).astype(jnp.int32)
        starts = jnp.concatenate([jnp.zeros((1,), jnp.int32), cut_flags, jnp.zeros((LEN - 1 - cut_span,), jnp.int32)])
        doc_ids = 1 + jnp.cumsum(starts).astype(jnp.int32)
        pad_count = jax.random.randint(key_pad, (), 1, LEN // 8 + 1)
        position = jnp.arange(LEN, dtype=jnp.int32)
        return jnp.where(position >= LEN - pad_count, 0, doc_ids).astype(jnp.int32)
    return jax.vmap(draw_single)(seq_keys).reshape(TOKENS)


def level_of(rng, dims, cuts, low, top_value):
    loudness = 1.0
    for axis_at, blocks in cuts:
        heights = jax.random.uniform(jax.random.fold_in(jax.random.fold_in(rng, 6), axis_at), (blocks,), jnp.float32, low / len(cuts), top_value / len(cuts))
        loudness = loudness * jnp.repeat(jnp.exp(heights), dims[axis_at] // blocks).reshape((-1,) + (1,) * (len(dims) - 1 - axis_at))
    return loudness


def centred(own_key, shape, scale, limit, pieces=(), kind=jnp.bfloat16):
    drawn = scale * jax.random.normal(own_key, shape, jnp.float32)
    if pieces:
        drawn = drawn * level_of(own_key, shape, pieces, -0.22, 0.18)
    return jnp.clip(drawn, -limit, limit).astype(kind)


def setup_inputs(seed: int = 0) -> dict:
    seeds = jax.random.split(jax.random.key(seed), 16)
    tokens = centred(seeds[0], (TOKENS, D), 1.0, 6.0, ((0, 32),))
    seg_ids = draw_seg_ids(jax.random.fold_in(seeds[15], 71), 0)
    gain_attn = jnp.clip(1.0 + 0.1 * jax.random.normal(seeds[2], (D,), jnp.float32), 0.5, 1.5).astype(jnp.bfloat16)
    w_query = centred(seeds[3], (D, D), (D // 2) ** -0.5, 0.21875, ((0, 16), (1, 2)))
    w_key = centred(seeds[4], (D, D), (D // 2) ** -0.5, 0.21875, ((0, 16), (1, 2)))
    w_value = centred(seeds[5], (D, D), D ** -0.5, 0.15625, ((0, 16), (1, 2)))
    w_outgate = centred(seeds[6], (D, D), D ** -0.5, 0.15625, ((0, 16), (1, 2)))
    w_forget = centred(seeds[7], (D, H), D ** -0.5, 0.15625, ((0, 16), (1, 2)))
    forget_bias = jnp.clip(1.0 + 6.0 * jax.random.uniform(seeds[8], (H,), jnp.float32) ** level_of(seeds[8], (H,), ((0, 2),), -0.2, 0.2), 1.0, 7.0).astype(jnp.bfloat16)
    w_out = centred(seeds[9], (D, D), (D // 32) ** -0.5, 0.875, ((0, 16), (1, 2)))
    gain_mlp = jnp.clip(1.0 + 0.1 * jax.random.normal(seeds[10], (D,), jnp.float32), 0.5, 1.5).astype(jnp.bfloat16)
    w_gate = centred(seeds[11], (D, FF), D ** -0.5, 0.15625, ((0, 16), (1, 2)))
    w_up = centred(seeds[12], (D, FF), D ** -0.5, 0.15625, ((0, 16), (1, 2)))
    w_down = centred(seeds[13], (D, FF), FF ** -0.5, 0.09375, ((0, 16), (1, 2)))
    grad_output = centred(seeds[14], (TOKENS, D), 1.0, 6.0, ((0, 32),))
    return dict(tokens=tokens, seg_ids=seg_ids, gain_attn=gain_attn, w_query=w_query, w_key=w_key, w_value=w_value, w_outgate=w_outgate, w_forget=w_forget, forget_bias=forget_bias, w_out=w_out, gain_mlp=gain_mlp, w_gate=w_gate, w_up=w_up, w_down=w_down, grad_output=grad_output)


epsilon = 1e-06

@jax.custom_vjp
def low(v):
    return lax.optimization_barrier(v.astype(jnp.bfloat16)).astype(jnp.float32)

@jax.custom_vjp
def low_back(v):
    return v

def low_keep(v):
    return (low(v), None)

def low_pass(kept, grad):
    return (grad,)

def back_keep(v):
    return (v, None)

def back_low(kept, grad):
    return (low(grad),)
low.defvjp(low_keep, low_pass)
low_back.defvjp(back_keep, back_low)

def matmul(left, right):
    return jnp.dot(left, right, precision=lax.Precision.HIGHEST, preferred_element_type=jnp.float32)

def matmul_nt(left, right):
    return lax.dot_general(left, right, (((1,), (1,)), ((), ())), precision=lax.Precision.HIGHEST, preferred_element_type=jnp.float32)

def rms_scale(values, gain):
    return values * lax.rsqrt(lax.optimization_barrier(jnp.mean(values * values, axis=-1, keepdims=True)) + epsilon) * gain

def attend(packed):
    queries, keys_in, values_in, cumulative, segments = packed
    position = jnp.arange(LEN, dtype=jnp.int32)
    allowed = (segments[:, None] == segments[None, :]) & (segments[None, :] != 0) & (position[None, :] <= position[:, None])
    allowed = allowed | (position[:, None] == position[None, :])
    logits = jnp.einsum('qhd,khd->hqk', queries, keys_in, precision=lax.Precision.HIGHEST) * HS ** (-0.5)
    logits = logits + cumulative.T[:, :, None] - cumulative.T[:, None, :]
    scores = jnp.where(allowed[None], low_back(logits), -1e+30)
    attn_probs = low(jax.nn.softmax(scores, axis=-1))
    return jnp.einsum('hqk,khd->qhd', attn_probs, values_in, precision=lax.Precision.HIGHEST)

def forward(tokens, gain_attn, w_query, w_key, w_value, w_outgate, w_forget, forget_bias, w_out, gain_mlp, w_gate, w_up, w_down, seg_ids):
    seq_count = tokens.shape[0] // LEN
    normed = low(rms_scale(tokens, gain_attn))
    queries = low_back(low(matmul(normed, w_query)))
    keys_all = low_back(low(matmul(normed, w_key)))
    values_all = low_back(low(matmul(normed, w_value)))
    gate_pre = low_back(matmul(normed, w_outgate))
    forget_pre = low_back(matmul(normed, w_forget) + forget_bias)
    cumulative = jnp.cumsum(jax.nn.log_sigmoid(forget_pre).reshape(seq_count, LEN, H), axis=1)
    head_shape = (seq_count, LEN, H, HS)
    attended = lax.map(jax.checkpoint(attend), (queries.reshape(head_shape), keys_all.reshape(head_shape), values_all.reshape(head_shape), cumulative, seg_ids.reshape(seq_count, LEN)))
    attended = low_back(attended.reshape(seq_count * LEN, D))
    gated = low(attended * jax.nn.sigmoid(gate_pre))
    hidden = tokens + low_back(matmul_nt(gated, w_out))
    normed_mlp = low(rms_scale(hidden, gain_mlp))
    gate_val = low_back(matmul(normed_mlp, w_gate))
    up_val = low_back(matmul(normed_mlp, w_up))
    mixed = low(jax.nn.silu(gate_val) * up_val)
    return hidden + low_back(matmul_nt(mixed, w_down))

def reference(tokens, seg_ids, gain_attn, w_query, w_key, w_value, w_outgate, w_forget, forget_bias, w_out, gain_mlp, w_gate, w_up, w_down, grad_output):
    floats = [array.astype(jnp.float32) for array in (tokens, gain_attn, w_query, w_key, w_value, w_outgate, w_forget, forget_bias, w_out, gain_mlp, w_gate, w_up, w_down)]

    def closed(*params):
        return forward(*params, seg_ids)
    output, pullback = jax.vjp(closed, *floats)
    grad_eff = jnp.where((seg_ids != 0)[:, None], grad_output.astype(jnp.float32), jnp.zeros_like(output))
    grads = pullback(grad_eff)
    return (output.astype(jnp.bfloat16), grads[0].astype(jnp.bfloat16), grads[1], grads[2], grads[3], grads[4], grads[5], grads[6], grads[7], grads[8], grads[9], grads[10], grads[11], grads[12])
```

```python
import functools

import jax
import jax.numpy as jnp
from jax import lax
from jax.experimental import pallas as pl
from jax.experimental.pallas import tpu as pltpu
from jax.sharding import PartitionSpec as P

LEN = 1024
epsilon = 1e-06


NEG = -1e30


def lane_split(value, head):
    lanes = lax.broadcasted_iota(jnp.int32, value.shape, 1)
    return lanes < 64 if head == 0 else lanes >= 64


def dot_nt(left, right):
    return lax.dot_general(
        left, right, (((1,), (1,)), ((), ())), preferred_element_type=jnp.float32
    )


def dot_tn(left, right):
    return lax.dot_general(
        left, right, (((0,), (0,)), ((), ())), preferred_element_type=jnp.float32
    )


def tile_allowed(start_row, height, first, width):
    key_pos = lax.broadcasted_iota(jnp.int32, (height, width), 0)
    query_pos = first + lax.broadcasted_iota(jnp.int32, (height, width), 1)
    return (key_pos >= start_row) & (key_pos <= query_pos)


def attend_forward_kernel(block, q_ref, k_ref, v_ref, ccol_ref, crow_ref, start_ref, o_ref, lse_ref):
    length = q_ref.shape[0]
    scale = jnp.asarray(0.125, jnp.bfloat16)
    for first in range(0, length, block):
        height = first + block
        query = q_ref[first : first + block, :] * scale
        start_row = start_ref[0, :, first : first + block]
        keys_all = k_ref[:height, :]
        values_all = v_ref[:height, :]
        outs = []
        for head in range(2):
            keys = jnp.where(lane_split(keys_all, head), keys_all, jnp.zeros_like(keys_all))
            logits = dot_nt(keys, query)
            logits = (logits + crow_ref[0, head : head + 1, first : first + block]) - ccol_ref[
                0, :height, head : head + 1
            ]
            logits = jnp.where(tile_allowed(start_row, height, first, block), logits, NEG)
            largest = jnp.max(logits, axis=0, keepdims=True)
            exponent = jnp.exp(logits - largest)
            total = jnp.sum(exponent, axis=0, keepdims=True)
            probs = (exponent * (1.0 / total)).astype(jnp.bfloat16)
            lse_ref[0, head : head + 1, first : first + block] = largest + jnp.log(total)
            outs.append(dot_tn(values_all, probs))
        rows = lax.broadcasted_iota(jnp.int32, outs[0].shape, 0)
        both = jnp.where(rows < 64, outs[0], outs[1])
        o_ref[first : first + block, :] = both.T


def attend_backward_kernel(
    block,
    q_ref,
    k_ref,
    v_ref,
    g_ref,
    ccol_ref,
    crow_ref,
    lse_ref,
    start_ref,
    dq_ref,
    dk_ref,
    dv_ref,
    row_ref,
    col_ref,
    dk_acc,
    dv_acc,
):
    length = q_ref.shape[0]
    scale = jnp.asarray(0.125, jnp.bfloat16)
    for first in reversed(range(0, length, block)):
        height = first + block
        top = height == length
        query = q_ref[first : first + block, :] * scale
        grad = g_ref[first : first + block, :]
        start_row = start_ref[0, :, first : first + block]
        keys_all = k_ref[:height, :]
        values_all = v_ref[:height, :]
        zeros = jnp.zeros_like(keys_all)
        outs = []
        for head in range(2):
            own = lane_split(keys_all, head)
            logits = dot_nt(jnp.where(own, keys_all, zeros), query)
            shift = (
                crow_ref[0, head : head + 1, first : first + block]
                - lse_ref[0, head : head + 1, first : first + block]
            )
            logits = (logits + shift) - ccol_ref[0, :height, head : head + 1]
            allowed = tile_allowed(start_row, height, first, block)
            probs = jnp.where(allowed, jnp.exp(logits), 0.0)
            grad_probs = dot_nt(jnp.where(own, values_all, zeros), grad)
            inner = jnp.sum(probs * grad_probs, axis=0, keepdims=True)
            grad_logits = (probs * (grad_probs - inner)).astype(jnp.bfloat16)
            low_probs = probs.astype(jnp.bfloat16)
            query_own = lane_split(query, head)
            one_query = jnp.where(query_own, query, jnp.ones_like(query))
            dk_part = jnp.dot(grad_logits, one_query, preferred_element_type=jnp.float32)
            dv_part = jnp.dot(low_probs, grad, preferred_element_type=jnp.float32)
            if top:
                dk_acc[head] = dk_part
                dv_acc[head] = dv_part
            else:
                dk_acc[head, :height, :] += dk_part
                dv_acc[head, :height, :] += dv_part
            out = dot_tn(jnp.where(own, keys_all, jnp.ones_like(keys_all)), grad_logits)
            other = 64 - 64 * head
            row_ref[0, head : head + 1, first : first + block] = out[other : other + 1, :]
            outs.append(out)
        rows = lax.broadcasted_iota(jnp.int32, outs[0].shape, 0)
        both = jnp.where(rows < 64, outs[0], outs[1]) * 0.125
        dq_ref[first : first + block, :] = both.T.astype(jnp.bfloat16)
    first_half = lane_split(dk_acc[0], 0)
    dk_ref[...] = jnp.where(first_half, dk_acc[0], dk_acc[1]).astype(jnp.bfloat16)
    dv_ref[...] = jnp.where(first_half, dv_acc[0], dv_acc[1]).astype(jnp.bfloat16)
    col_ref[0, :, 0:1] = dk_acc[0, :, 64:65]
    col_ref[0, :, 1:2] = dk_acc[1, :, 0:1]


def attention_specs(length, pairs):
    wide = pl.BlockSpec((length, 128), lambda s, p: (s, p))
    column = pl.BlockSpec((1, length, 2), lambda s, p: (s * pairs + p, 0, 0))
    row = pl.BlockSpec((1, 2, length), lambda s, p: (s * pairs + p, 0, 0))
    start = pl.BlockSpec((1, 1, length), lambda s, p: (s, 0, 0))
    return wide, column, row, start


def attend_forward(queries, keys, values, ccol, crow, start):
    seqs, _, length = start.shape
    pairs = queries.shape[1] // 128
    wide, column, row, first = attention_specs(length, pairs)
    tiles = seqs * pairs
    cost = pl.CostEstimate(
        flops=tiles * length * length * 512, bytes_accessed=queries.size * 10, transcendentals=tiles * length * length
    )
    return pl.pallas_call(
        functools.partial(attend_forward_kernel, min(256, length)),
        grid=(seqs, pairs),
        in_specs=[wide, wide, wide, column, row, first],
        out_specs=[wide, row],
        out_shape=[
            jax.ShapeDtypeStruct(queries.shape, jnp.float32),
            jax.ShapeDtypeStruct((tiles, 2, length), jnp.float32),
        ],
        compiler_params=pltpu.CompilerParams(vmem_limit_bytes=48 << 20),
        cost_estimate=cost,
        name="attend_forward",
    )(queries, keys, values, ccol, crow, start)


def attend_backward(queries, keys, values, grad, ccol, crow, lse, start):
    seqs, _, length = start.shape
    pairs = queries.shape[1] // 128
    wide, column, row, first = attention_specs(length, pairs)
    tiles = seqs * pairs
    cost = pl.CostEstimate(
        flops=tiles * length * length * 1280, bytes_accessed=queries.size * 14, transcendentals=tiles * length * length
    )
    low = jax.ShapeDtypeStruct(queries.shape, jnp.bfloat16)
    return pl.pallas_call(
        functools.partial(attend_backward_kernel, min(256, length)),
        grid=(seqs, pairs),
        in_specs=[wide, wide, wide, wide, column, row, row, first],
        out_specs=[wide, wide, wide, row, column],
        out_shape=[
            low,
            low,
            low,
            jax.ShapeDtypeStruct((tiles, 2, length), jnp.float32),
            jax.ShapeDtypeStruct((tiles, length, 2), jnp.float32),
        ],
        scratch_shapes=[
            pltpu.VMEM((2, length, 128), jnp.float32),
            pltpu.VMEM((2, length, 128), jnp.float32),
        ],
        compiler_params=pltpu.CompilerParams(vmem_limit_bytes=48 << 20),
        cost_estimate=cost,
        name="attend_backward",
    )(queries, keys, values, grad, ccol, crow, lse, start)


def to_low(value):
    return value.astype(jnp.bfloat16)


def dot_plain(left, right):
    return jnp.dot(left, right, preferred_element_type=jnp.float32)


dot_rows = dot_nt
dot_cols = dot_tn


def norm_forward(values, gain):
    inverse = lax.rsqrt(jnp.mean(values * values, axis=-1, keepdims=True) + epsilon)
    unit_rows = values * inverse
    return (unit_rows, inverse, unit_rows * gain)


def norm_backward(grad_normed, unit_rows, inverse, gain):
    grad_unit = grad_normed * gain
    centred = grad_unit - unit_rows * jnp.mean(grad_unit * unit_rows, axis=-1, keepdims=True)
    return (inverse * centred, jnp.sum(grad_normed * unit_rows, axis=0))


SWAP = [(0, 1), (1, 0)]


def join_halves(own, side):
    other = lax.ppermute(own, "tensor", SWAP)
    first = jnp.where(side == 0, own, other)
    second = jnp.where(side == 0, other, own)
    return jnp.concatenate([first, second], axis=0)


def sum_halves(terms, side):
    rows = terms.shape[0] // 2
    away = lax.dynamic_slice_in_dim(terms, (1 - side) * rows, rows, 0)
    arrived = lax.ppermute(to_low(away), "tensor", SWAP)
    return lax.dynamic_slice_in_dim(terms, side * rows, rows, 0) + arrived.astype(jnp.float32)


def document_starts(segments):
    position = jnp.arange(segments.shape[-1], dtype=jnp.int32)
    before = (segments[..., None, :] != segments[..., :, None]) & (position[None, :] < position[:, None])
    starts = jnp.sum(before, axis=-1, dtype=jnp.int32)
    return jnp.where(segments != 0, starts, position)


def local(
    tokens,
    seg_ids,
    gain_attn,
    w_query,
    w_key,
    w_value,
    w_outgate,
    w_forget,
    forget_bias,
    w_out,
    gain_mlp,
    w_gate,
    w_up,
    w_down,
    grad_output,
):
    row_count, width = tokens.shape
    seq_count = seg_ids.shape[0] // LEN
    side = lax.axis_index("tensor")
    cols = w_query.shape[1]
    head_count = w_forget.shape[1]
    hidden_cols = w_gate.shape[1]
    pad = 128 - head_count - 2
    packed = jnp.concatenate(
        [
            w_query,
            w_key,
            w_value,
            w_outgate,
            w_forget,
            gain_attn[:, None],
            gain_mlp[:, None],
            jnp.zeros((w_query.shape[0], pad), jnp.bfloat16),
        ],
        axis=1,
    )
    attn_mat = lax.all_gather(packed, "dp", axis=0, tiled=True)
    rest = jnp.concatenate([w_out, w_gate, w_up, w_down], axis=1)
    rest_mat = lax.all_gather(rest, "dp", axis=0, tiled=True)
    out_mat = rest_mat[:, :cols]
    gate_mat = rest_mat[:, cols : cols + hidden_cols]
    up_mat = rest_mat[:, cols + hidden_cols : cols + 2 * hidden_cols]
    down_mat = rest_mat[:, cols + 2 * hidden_cols :]
    gains = attn_mat[:, 4 * cols + head_count : 4 * cols + head_count + 2].astype(jnp.float32).T
    attn_gain, mlp_gain = gains[0], gains[1]

    residual = tokens.astype(jnp.float32)
    unit_attn, inv_attn, normed = norm_forward(residual, attn_gain)
    normed_all = join_halves(to_low(normed), side)
    query_rows = to_low(dot_plain(normed_all, attn_mat[:, :cols]))
    key_rows = to_low(dot_plain(normed_all, attn_mat[:, cols : 2 * cols]))
    value_rows = to_low(dot_plain(normed_all, attn_mat[:, 2 * cols : 3 * cols]))
    gate_pre = dot_plain(normed_all, attn_mat[:, 3 * cols : 4 * cols])
    forget_pre = dot_plain(normed_all, attn_mat[:, 4 * cols :])[:, :head_count] + forget_bias.astype(
        jnp.float32
    )
    cumulative = jnp.cumsum(
        jax.nn.log_sigmoid(forget_pre).reshape(seq_count, LEN, head_count), axis=1
    )
    pairs = head_count // 2
    tiles = seq_count * pairs
    paired = cumulative.reshape(seq_count, LEN, pairs, 2)
    ccol = paired.transpose(0, 2, 1, 3).reshape(tiles, LEN, 2)
    crow = paired.transpose(0, 2, 3, 1).reshape(tiles, 2, LEN)
    start = document_starts(seg_ids.reshape(seq_count, LEN))[:, None, :]
    attended, lse = attend_forward(query_rows, key_rows, value_rows, ccol, crow, start)
    out_gate = jax.nn.sigmoid(gate_pre)
    gated = to_low(attended * out_gate)
    hidden = residual + sum_halves(dot_rows(gated, out_mat), side)
    unit_mlp, inv_mlp, normed_mlp = norm_forward(hidden, mlp_gain)
    normed_mlp_all = join_halves(to_low(normed_mlp), side)
    gate_val = dot_plain(normed_mlp_all, gate_mat)
    up_val = dot_plain(normed_mlp_all, up_mat)
    sig_gate = jax.nn.sigmoid(gate_val)
    mixed = to_low(gate_val * sig_gate * up_val)
    output = hidden + sum_halves(dot_rows(mixed, down_mat), side)

    own_segs = lax.dynamic_slice_in_dim(seg_ids, side * row_count, row_count, 0)
    grad_y = jnp.where((own_segs != 0)[:, None], grad_output, jnp.zeros_like(grad_output))
    grad_y_all = join_halves(grad_y, side)
    grad_down = to_low(dot_cols(grad_y_all, mixed))
    grad_mixed = dot_plain(grad_y_all, down_mat)
    grad_gate = to_low(grad_mixed * up_val * sig_gate * (1.0 + gate_val * (1.0 - sig_gate)))
    grad_upval = to_low(grad_mixed * gate_val * sig_gate)
    grad_gate_mat = to_low(dot_cols(normed_mlp_all, grad_gate))
    grad_up_mat = to_low(dot_cols(normed_mlp_all, grad_upval))
    mlp_grads = jnp.concatenate([grad_gate_mat, grad_up_mat, grad_down], axis=1)
    mlp_sent = lax.psum_scatter(mlp_grads, "dp", scatter_dimension=0, tiled=True)
    mlp_in_terms = dot_rows(grad_gate, gate_mat) + dot_rows(grad_upval, up_mat)
    grad_normed_mlp = sum_halves(mlp_in_terms, side)
    back_mlp, gain_mlp_part = norm_backward(grad_normed_mlp, unit_mlp, inv_mlp, mlp_gain)
    grad_hidden = grad_y.astype(jnp.float32) + back_mlp
    grad_attn_all = join_halves(to_low(grad_hidden), side)
    grad_out_mat = to_low(dot_cols(grad_attn_all, gated))
    grad_gated = dot_plain(grad_attn_all, out_mat)
    grad_attended = to_low(grad_gated * out_gate)
    grad_gate_pre = to_low(grad_gated * attended * out_gate * (1.0 - out_gate))
    grad_q, grad_k, grad_v, row_part, col_part = attend_backward(
        query_rows, key_rows, value_rows, grad_attended, ccol, crow, lse, start
    )
    flat_rows = seq_count * LEN
    grad_cumul = row_part.reshape(seq_count, pairs, 2, LEN).transpose(0, 3, 1, 2) - col_part.reshape(
        seq_count, pairs, LEN, 2
    ).transpose(0, 2, 1, 3)
    grad_cumul = grad_cumul.reshape(seq_count, LEN, head_count)
    grad_logf = jnp.flip(jnp.cumsum(jnp.flip(grad_cumul, 1), axis=1), 1)
    grad_forget_pre = to_low(grad_logf.reshape(flat_rows, head_count) * jax.nn.sigmoid(-forget_pre))
    forget_pad = jnp.pad(grad_forget_pre, ((0, 0), (0, 128 - head_count)))
    grad_parts = (grad_q, grad_k, grad_v, grad_gate_pre, forget_pad)
    attn_grads = jnp.concatenate(
        [grad_out_mat] + [to_low(dot_cols(normed_all, part)) for part in grad_parts], axis=1
    )
    attn_sent = lax.psum_scatter(attn_grads, "dp", scatter_dimension=0, tiled=True)
    bias_part = jnp.sum(grad_forget_pre, axis=0, dtype=jnp.float32)
    attn_in_terms = dot_rows(jnp.concatenate(grad_parts, axis=1), attn_mat)
    grad_normed_attn = sum_halves(attn_in_terms, side)
    back_attn, gain_attn_part = norm_backward(grad_normed_attn, unit_attn, inv_attn, attn_gain)
    grad_tokens = to_low(grad_hidden + back_attn)
    slots = lax.dynamic_update_slice_in_dim(
        jnp.zeros((lax.axis_size("tensor") * head_count,), jnp.float32), bias_part, side * head_count, 0
    )
    small = lax.psum(jnp.concatenate([gain_attn_part, gain_mlp_part, slots]), ("dp", "tensor"))
    own = gain_attn.shape[0]
    at = lax.axis_index("dp") * own
    gain_attn_grad = lax.dynamic_slice_in_dim(small, at, own, 0)
    gain_mlp_grad = lax.dynamic_slice_in_dim(small, width + at, own, 0)
    bias_grad = lax.dynamic_slice_in_dim(small, 2 * width + side * head_count, head_count, 0)
    attn_sent = attn_sent.astype(jnp.float32)
    mlp_sent = mlp_sent.astype(jnp.float32)
    return (
        to_low(output),
        grad_tokens,
        gain_attn_grad,
        attn_sent[:, cols : 2 * cols],
        attn_sent[:, 2 * cols : 3 * cols],
        attn_sent[:, 3 * cols : 4 * cols],
        attn_sent[:, 4 * cols : 5 * cols],
        attn_sent[:, 5 * cols : 5 * cols + head_count],
        bias_grad,
        attn_sent[:, :cols],
        gain_mlp_grad,
        mlp_sent[:, :hidden_cols],
        mlp_sent[:, hidden_cols : 2 * hidden_cols],
        mlp_sent[:, 2 * hidden_cols :],
    )


def solution(mesh):
    placed = (
        P(("dp", "tensor"), None),
        P("dp"),
        P("dp"),
        P("dp", "tensor"),
        P("dp", "tensor"),
        P("dp", "tensor"),
        P("dp", "tensor"),
        P("dp", "tensor"),
        P("tensor"),
        P("dp", "tensor"),
        P("dp"),
        P("dp", "tensor"),
        P("dp", "tensor"),
        P("dp", "tensor"),
        P(("dp", "tensor"), None),
    )
    return jax.shard_map(
        local,
        mesh=mesh,
        in_specs=placed,
        out_specs=(
            P(("dp", "tensor"), None),
            P(("dp", "tensor"), None),
            P("dp"),
            P("dp", "tensor"),
            P("dp", "tensor"),
            P("dp", "tensor"),
            P("dp", "tensor"),
            P("dp", "tensor"),
            P("tensor"),
            P("dp", "tensor"),
            P("dp"),
            P("dp", "tensor"),
            P("dp", "tensor"),
            P("dp", "tensor"),
        ),
        check_vma=False,
    )
```

```python
import functools

import jax
import jax.numpy as jnp
from jax import lax
from jax.experimental import pallas as pl
from jax.experimental.pallas import tpu as pltpu
from jax.sharding import PartitionSpec as P

LEN = 1024
epsilon = 1e-06


NEG = -1e30


def lane_split(value, head):
    lanes = lax.broadcasted_iota(jnp.int32, value.shape, 1)
    return lanes < 64 if head == 0 else lanes >= 64


def dot_nt(left, right):
    return lax.dot_general(
        left, right, (((1,), (1,)), ((), ())), preferred_element_type=jnp.float32
    )


def dot_tn(left, right):
    return lax.dot_general(
        left, right, (((0,), (0,)), ((), ())), preferred_element_type=jnp.float32
    )


def tile_allowed(start_row, height, first, width):
    key_pos = lax.broadcasted_iota(jnp.int32, (height, width), 0)
    query_pos = first + lax.broadcasted_iota(jnp.int32, (height, width), 1)
    return (key_pos >= start_row) & (key_pos <= query_pos)


def column_of(crow_ref):
    rows = crow_ref[0]
    return jnp.concatenate([rows, jnp.zeros((6, rows.shape[1]), rows.dtype)], axis=0).T


def attend_forward_kernel(block, qkv_ref, crow_ref, start_ref, o_ref, lse_ref):
    length = qkv_ref.shape[0]
    scale = jnp.asarray(0.125, jnp.bfloat16)
    ccol = column_of(crow_ref)
    for first in range(0, length, block):
        height = first + block
        query = qkv_ref[first : first + block, :128] * scale
        start_row = start_ref[0, :, first : first + block]
        keys_all = qkv_ref[:height, 128:256]
        values_all = qkv_ref[:height, 256:]
        allowed = tile_allowed(start_row, height, first, block)
        outs = []
        for head in range(2):
            keys = jnp.where(lane_split(keys_all, head), keys_all, jnp.zeros_like(keys_all))
            logits = dot_nt(keys, query)
            shift = crow_ref[0, head : head + 1, first : first + block]
            logits = (logits + shift) - ccol[:height, head : head + 1]
            logits = jnp.where(allowed, logits, NEG)
            largest = jnp.max(logits, axis=0, keepdims=True)
            exponent = jnp.exp(logits - largest)
            total = jnp.sum(exponent, axis=0, keepdims=True)
            probs = (exponent * (1.0 / total)).astype(jnp.bfloat16)
            lse_ref[0, head : head + 1, first : first + block] = largest + jnp.log(total)
            outs.append(dot_tn(values_all, probs))
        rows = lax.broadcasted_iota(jnp.int32, outs[0].shape, 0)
        both = jnp.where(rows < 64, outs[0], outs[1])
        o_ref[first : first + block, :] = both.T


def attend_backward_kernel(
    block, qkv_ref, g_ref, crow_ref, lse_ref, start_ref, d_ref, cumul_ref, dk_acc, dv_acc
):
    length = qkv_ref.shape[0]
    scale = jnp.asarray(0.125, jnp.bfloat16)
    ccol = column_of(crow_ref)
    for first in reversed(range(0, length, block)):
        height = first + block
        top = height == length
        query = qkv_ref[first : first + block, :128] * scale
        grad = g_ref[first : first + block, :]
        start_row = start_ref[0, :, first : first + block]
        keys_all = qkv_ref[:height, 128:256]
        values_all = qkv_ref[:height, 256:]
        allowed = tile_allowed(start_row, height, first, block)
        zeros = jnp.zeros_like(keys_all)
        outs = []
        for head in range(2):
            own = lane_split(keys_all, head)
            logits = dot_nt(jnp.where(own, keys_all, zeros), query)
            shift = (
                crow_ref[0, head : head + 1, first : first + block]
                - lse_ref[0, head : head + 1, first : first + block]
            )
            logits = (logits + shift) - ccol[:height, head : head + 1]
            probs = jnp.where(allowed, jnp.exp(logits), 0.0)
            grad_probs = dot_nt(jnp.where(own, values_all, zeros), grad)
            inner = jnp.sum(probs * grad_probs, axis=0, keepdims=True)
            grad_logits = (probs * (grad_probs - inner)).astype(jnp.bfloat16)
            low_probs = probs.astype(jnp.bfloat16)
            query_own = lane_split(query, head)
            one_query = jnp.where(query_own, query, jnp.ones_like(query))
            dk_part = jnp.dot(grad_logits, one_query, preferred_element_type=jnp.float32)
            dv_part = jnp.dot(low_probs, grad, preferred_element_type=jnp.float32)
            if top:
                dk_acc[head] = dk_part
                dv_acc[head] = dv_part
            else:
                dk_acc[head, :height, :] += dk_part
                dv_acc[head, :height, :] += dv_part
            out = dot_tn(jnp.where(own, keys_all, jnp.ones_like(keys_all)), grad_logits)
            other = 64 - 64 * head
            cumul_ref[0, head : head + 1, first : first + block] = out[other : other + 1, :]
            outs.append(out)
        rows = lax.broadcasted_iota(jnp.int32, outs[0].shape, 0)
        both = jnp.where(rows < 64, outs[0], outs[1]) * 0.125
        d_ref[first : first + block, :128] = both.T.astype(jnp.bfloat16)
    keys_one, keys_two = dk_acc[0], dk_acc[1]
    first_half = lane_split(keys_one, 0)
    d_ref[:, 128:256] = jnp.where(first_half, keys_one, keys_two).astype(jnp.bfloat16)
    d_ref[:, 256:] = jnp.where(first_half, dv_acc[0], dv_acc[1]).astype(jnp.bfloat16)
    sums = jnp.where(first_half, keys_two, keys_one).T
    cumul_ref[0, 0:1, :] -= sums[64:65, :]
    cumul_ref[0, 1:2, :] -= sums[0:1, :]


def attention_specs(length, pairs, at=0):
    triple = pl.BlockSpec((length, 384), lambda s, p: (s, p + at))
    wide = pl.BlockSpec((length, 128), lambda s, p: (s, p + at))
    row = pl.BlockSpec((1, 2, length), lambda s, p: (s * pairs + p + at, 0, 0))
    start = pl.BlockSpec((1, 1, length), lambda s, p: (s, 0, 0))
    return triple, wide, row, start


def attend_forward(qkv, crow, start):
    seqs, _, length = start.shape
    pairs = qkv.shape[1] // 384
    triple, wide, row, first = attention_specs(length, pairs)
    tiles = seqs * pairs
    work = tiles * length * length
    cost = pl.CostEstimate(flops=work * 512, bytes_accessed=qkv.size * 4, transcendentals=work)
    return pl.pallas_call(
        functools.partial(attend_forward_kernel, min(256, length)),
        grid=(seqs, pairs),
        in_specs=[triple, row, first],
        out_specs=[wide, row],
        out_shape=[
            jax.ShapeDtypeStruct((qkv.shape[0], pairs * 128), jnp.float32),
            jax.ShapeDtypeStruct((tiles, 2, length), jnp.float32),
        ],
        compiler_params=pltpu.CompilerParams(vmem_limit_bytes=48 << 20),
        cost_estimate=cost,
        name="attend_forward",
    )(qkv, crow, start)


def attend_backward(qkv, grad, crow, lse, start, at, count):
    seqs, _, length = start.shape
    pairs = qkv.shape[1] // 384
    triple, wide, row, first = attention_specs(length, pairs, at)
    triple_out, _, row_out, _ = attention_specs(length, count)
    tiles = seqs * count
    work = tiles * length * length
    cost = pl.CostEstimate(flops=work * 1280, bytes_accessed=tiles * length * 2000, transcendentals=work)
    return pl.pallas_call(
        functools.partial(attend_backward_kernel, min(256, length)),
        grid=(seqs, count),
        in_specs=[triple, wide, row, row, first],
        out_specs=[triple_out, row_out],
        out_shape=[
            jax.ShapeDtypeStruct((qkv.shape[0], count * 384), jnp.bfloat16),
            jax.ShapeDtypeStruct((tiles, 2, length), jnp.float32),
        ],
        scratch_shapes=[
            pltpu.VMEM((2, length, 128), jnp.float32),
            pltpu.VMEM((2, length, 128), jnp.float32),
        ],
        compiler_params=pltpu.CompilerParams(vmem_limit_bytes=48 << 20),
        cost_estimate=cost,
        name="attend_backward",
    )(qkv, grad, crow, lse, start)


def to_low(value):
    return value.astype(jnp.bfloat16)


def dot_plain(left, right):
    return jnp.dot(left, right, preferred_element_type=jnp.float32)


dot_rows = dot_nt
dot_cols = dot_tn


def norm_forward(values, gain):
    inverse = lax.rsqrt(jnp.mean(values * values, axis=-1, keepdims=True) + epsilon)
    unit_rows = values * inverse
    return (unit_rows, inverse, unit_rows * gain)


def norm_backward(grad_normed, unit_rows, inverse, gain):
    grad_unit = grad_normed * gain
    centred = grad_unit - unit_rows * jnp.mean(grad_unit * unit_rows, axis=-1, keepdims=True)
    return (inverse * centred, jnp.sum(grad_normed * unit_rows, axis=0))


SWAP = [(0, 1), (1, 0)]


def order_halves(own, other, side):
    first = jnp.where(side == 0, own, other)
    second = jnp.where(side == 0, other, own)
    return jnp.concatenate([first, second], axis=0)


def join_halves(own, side):
    return order_halves(own, lax.ppermute(own, "tensor", SWAP), side)


def thirds(values):
    parts = []
    for _ in range(3):
        part = lax.reduce_precision(values, 8, 7)
        parts.append(to_low(part))
        values = values - part
    return parts


def sum_thirds(product, axis):
    first, second, third = jnp.split(product, 3, axis=axis)
    return (third + second) + first


def split_halves(terms, side):
    rows = terms.shape[0] // 2
    away = lax.dynamic_slice_in_dim(terms, (1 - side) * rows, rows, 0)
    arrived = lax.ppermute(to_low(away), "tensor", SWAP)
    return lax.dynamic_slice_in_dim(terms, side * rows, rows, 0), arrived


def sum_halves(terms, side):
    kept, arrived = split_halves(terms, side)
    return kept + arrived.astype(jnp.float32)


def width_cut(columns):
    return (columns // 2 + 127) // 128 * 128


def document_starts(segments):
    position = jnp.arange(segments.shape[-1], dtype=jnp.int32)
    before = (segments[..., None, :] != segments[..., :, None]) & (position[None, :] < position[:, None])
    starts = jnp.sum(before, axis=-1, dtype=jnp.int32)
    return jnp.where(segments != 0, starts, position)


def local(
    tokens,
    seg_ids,
    gain_attn,
    w_query,
    w_key,
    w_value,
    w_outgate,
    w_forget,
    forget_bias,
    w_out,
    gain_mlp,
    w_gate,
    w_up,
    w_down,
    grad_output,
):
    row_count, width = tokens.shape
    seq_count = seg_ids.shape[0] // LEN
    side = lax.axis_index("tensor")
    cols = w_query.shape[1]
    head_count = w_forget.shape[1]
    hidden_cols = w_gate.shape[1]
    pad = 128 - head_count - 2
    shard = w_query.shape[0]
    pairs = head_count // 2
    triples = jnp.stack([w.reshape(shard, pairs, 128) for w in (w_query, w_key, w_value)], axis=2)
    packed = jnp.concatenate(
        [
            triples.reshape(shard, 3 * cols),
            w_outgate,
            w_out,
            w_forget,
            gain_attn[:, None],
            gain_mlp[:, None],
            jnp.zeros((shard, pad), jnp.bfloat16),
        ],
        axis=1,
    )
    attn_mat = lax.all_gather(packed, "dp", axis=0, tiled=True)
    qkv_mat = attn_mat[:, : 3 * cols]
    ogate_mat = attn_mat[:, 3 * cols : 4 * cols]
    out_mat = attn_mat[:, 4 * cols : 5 * cols]
    forget_mat = attn_mat[:, 5 * cols :]
    rest = jnp.concatenate([w_gate, w_up, w_down], axis=1)
    rest_mat = lax.all_gather(rest, "dp", axis=0, tiled=True)
    gate_mat = rest_mat[:, :hidden_cols]
    up_mat = rest_mat[:, hidden_cols : 2 * hidden_cols]
    down_mat = rest_mat[:, 2 * hidden_cols :]
    gains = forget_mat[:, head_count : head_count + 2].astype(jnp.float32).T
    attn_gain, mlp_gain = gains[0], gains[1]

    tokens_away = lax.ppermute(tokens, "tensor", SWAP)
    grad_away = lax.ppermute(grad_output, "tensor", SWAP)
    tokens_away, grad_away = lax.optimization_barrier((tokens_away, grad_away))
    tokens_all = order_halves(tokens, tokens_away, side).astype(jnp.float32)
    normed_all = to_low(norm_forward(tokens_all, attn_gain)[2])
    qkv = to_low(dot_plain(normed_all, qkv_mat))
    gate_pre = dot_plain(normed_all, ogate_mat)
    forget_pre = dot_plain(normed_all, forget_mat)[:, :head_count] + forget_bias.astype(jnp.float32)
    position = jnp.arange(LEN, dtype=jnp.int32)
    upto = to_low(position[:, None] <= position[None, :])
    logs = jax.nn.log_sigmoid(forget_pre).reshape(seq_count, LEN, head_count)
    crow = sum_thirds(
        jnp.einsum("psh,si->phi", jnp.concatenate(thirds(logs), axis=2), upto, preferred_element_type=jnp.float32),
        1,
    ).reshape(seq_count * pairs, 2, LEN)
    start = document_starts(seg_ids.reshape(seq_count, LEN))[:, None, :]
    attended, lse = attend_forward(qkv, crow, start)
    residual = tokens.astype(jnp.float32)
    out_gate = jax.nn.sigmoid(gate_pre)
    gated = to_low(attended * out_gate)
    hidden = residual + sum_halves(dot_rows(gated, out_mat), side)
    unit_mlp, inv_mlp, normed_mlp = norm_forward(hidden, mlp_gain)
    normed_mlp_all = join_halves(to_low(normed_mlp), side)
    gate_val = dot_plain(normed_mlp_all, gate_mat)
    up_val = dot_plain(normed_mlp_all, up_mat)
    sig_gate = jax.nn.sigmoid(gate_val)
    mixed = to_low(gate_val * sig_gate * up_val)
    output = hidden + sum_halves(dot_rows(mixed, down_mat), side)

    grad_all = order_halves(grad_output, grad_away, side)
    grad_y_all = jnp.where((seg_ids != 0)[:, None], grad_all, jnp.zeros_like(grad_all))
    grad_y = lax.dynamic_slice_in_dim(grad_y_all, side * row_count, row_count, 0)
    down_terms = to_low(dot_cols(grad_y_all, mixed))
    half = width_cut(down_terms.shape[1])
    down_one, down_two = Ring(down_terms[:, :half], 1), Ring(down_terms[:, half:], -1)
    grad_mixed = dot_plain(grad_y_all, down_mat)
    grad_gate = to_low(grad_mixed * up_val * sig_gate * (1.0 + gate_val * (1.0 - sig_gate)))
    grad_upval = to_low(grad_mixed * gate_val * sig_gate)
    grad_gate, grad_upval = tie((grad_gate, grad_upval), down_one, down_two)
    hop_all(down_one, down_two)
    mlp_in_terms = dot_rows(grad_gate, gate_mat) + dot_rows(grad_upval, up_mat)
    mlp_in_terms, grad_gate = tie((mlp_in_terms, grad_gate), down_one, down_two)
    kept, arrived = split_halves(mlp_in_terms, side)
    hop_all(down_one, down_two)
    grad_gate_mat = to_low(dot_cols(normed_mlp_all, grad_gate))
    grad_gate_mat, grad_upval = tie((grad_gate_mat, grad_upval), down_one, down_two)
    gate_ring = Ring(grad_gate_mat, 1)
    hop_all(down_one, down_two)
    grad_up_mat = to_low(dot_cols(normed_mlp_all, grad_upval))
    grad_up_mat, arrived = tie((grad_up_mat, arrived), gate_ring, down_one, down_two)
    up_ring = Ring(grad_up_mat, -1)
    grad_normed_mlp = kept + arrived.astype(jnp.float32)
    back_mlp, gain_mlp_part = norm_backward(grad_normed_mlp, unit_mlp, inv_mlp, mlp_gain)
    grad_hidden = grad_y.astype(jnp.float32) + back_mlp
    attn_own = to_low(grad_hidden)
    attn_own = tie(attn_own, gate_ring, up_ring)
    attn_away = lax.ppermute(attn_own, "tensor", SWAP)
    for _ in range(2):
        hop_all(down_one, down_two, gate_ring, up_ring)
    hop_all(down_one, down_two)
    attn_own, attn_away = tie((attn_own, attn_away), down_one, down_two, gate_ring, up_ring)
    grad_attn_all = order_halves(attn_own, attn_away, side)
    hop_all(down_one, down_two, gate_ring, up_ring)
    grad_gated = dot_plain(grad_attn_all, out_mat)
    grad_attended = to_low(grad_gated * out_gate)
    grad_gate_pre = to_low(grad_gated * attended * out_gate * (1.0 - out_gate))
    grad_attended, grad_gate_pre = tie((grad_attended, grad_gate_pre), gate_ring, up_ring)
    hop_all(gate_ring, up_ring)
    grad_out_mat = to_low(dot_cols(grad_attn_all, gated))
    grad_ogate_mat = to_low(dot_cols(normed_all, grad_gate_pre))
    grad_attended, grad_out_mat, grad_ogate_mat = tie(
        (grad_attended, grad_out_mat, grad_ogate_mat), gate_ring, up_ring
    )
    out_ring, ogate_ring = Ring(grad_out_mat, 1), Ring(grad_ogate_mat, -1)
    hop_all(gate_ring, up_ring)
    lower = pairs // 2
    grad_one, cumul_one = attend_backward(qkv, grad_attended, crow, lse, start, 0, lower)
    grad_one, grad_attended = tie(
        (grad_one, grad_attended), gate_ring, up_ring, out_ring, ogate_ring
    )
    hop_all(gate_ring, up_ring, out_ring, ogate_ring)
    grad_two, cumul_two = attend_backward(
        qkv, grad_attended, crow, lse, start, lower, pairs - lower
    )
    one_ring = Ring(to_low(dot_cols(normed_all, grad_one)), 1)
    grad_two, grad_one = tie((grad_two, grad_one), gate_ring, up_ring, out_ring, ogate_ring)
    two_ring = Ring(to_low(dot_cols(normed_all, grad_two)), -1)
    terms = dot_rows(grad_gate_pre, ogate_mat) + dot_rows(grad_one, qkv_mat[:, : 384 * lower])
    terms = terms + dot_rows(grad_two, qkv_mat[:, 384 * lower :])

    cumuls = [c.reshape(seq_count, -1, LEN) for c in (cumul_one, cumul_two)]
    grad_cumul = jnp.concatenate(cumuls, axis=1)
    grad_logf = sum_thirds(
        jnp.einsum(
            "phi,si->psh",
            jnp.concatenate(thirds(grad_cumul), axis=1),
            upto,
            preferred_element_type=jnp.float32,
        ),
        2,
    )
    flat_rows = seq_count * LEN
    grad_forget_pre = to_low(grad_logf.reshape(flat_rows, head_count) * jax.nn.sigmoid(-forget_pre))
    forget_pad = jnp.pad(grad_forget_pre, ((0, 0), (0, 128 - head_count)))
    terms = terms + dot_rows(forget_pad, forget_mat)
    kept, arrived = split_halves(terms, side)
    unit_all, _, _ = norm_forward(tokens_all, attn_gain)
    gain_attn_part = jnp.sum(terms * unit_all, axis=0)
    bias_part = jnp.sum(grad_forget_pre, axis=0, dtype=jnp.float32)
    small = jnp.concatenate(
        [
            dot_cols(normed_all, forget_pad)[:, :head_count],
            gain_attn_part[:, None],
            gain_mlp_part[:, None],
            jnp.broadcast_to(bias_part[None], (width, head_count)),
            jnp.zeros((width, 126 - 2 * head_count), jnp.float32),
        ],
        axis=1,
    )
    small_ring = Ring(small, 1)
    hop_all(gate_ring, up_ring, out_ring, ogate_ring)
    for _ in range(small_ring.chips - 1):
        hop_all(one_ring, two_ring, out_ring, ogate_ring, small_ring)
    grad_normed_attn = kept + arrived.astype(jnp.float32)
    unit_attn, inv_attn, _ = norm_forward(residual, attn_gain)
    back_attn, _ = norm_backward(grad_normed_attn, unit_attn, inv_attn, attn_gain)
    grad_tokens = to_low(grad_hidden + back_attn)
    small_sent = small_ring.finish()
    gains = small_sent[:, head_count : head_count + 2]
    gains = gains + lax.ppermute(gains, "tensor", SWAP)
    bias_grad = small_sent[0, head_count + 2 : 2 * head_count + 2]
    qkv_sent = jnp.concatenate(
        [
            one_ring.finish().reshape(shard, lower, 3, 128),
            two_ring.finish().reshape(shard, pairs - lower, 3, 128),
        ],
        axis=1,
    )
    return (
        to_low(output),
        grad_tokens,
        gains[:, 0],
        qkv_sent[:, :, 0].reshape(shard, cols),
        qkv_sent[:, :, 1].reshape(shard, cols),
        qkv_sent[:, :, 2].reshape(shard, cols),
        ogate_ring.finish(),
        small_sent[:, :head_count],
        bias_grad,
        out_ring.finish(),
        gains[:, 1],
        gate_ring.finish(),
        up_ring.finish(),
        jnp.concatenate([down_one.finish(), down_two.finish()], axis=1),
    )


def chip_at(position, chips):
    half = chips // 2
    return jnp.where(position < half, 2 * position, 2 * (chips - 1 - position) + 1)


def ring_pairs(chips, step):
    half = chips // 2
    order = [2 * p if p < half else 2 * (chips - 1 - p) + 1 for p in range(chips)]
    pairs = []
    for place, chip in enumerate(order):
        target = order[(place + step) % chips]
        pairs += [(2 * chip + core, 2 * target + core) for core in range(2)]
    return pairs


class Ring:
    def __init__(self, grads, step):
        size = lax.axis_size("dp")
        self.chips = size // 2
        self.step = step
        self.low = grads.dtype
        index = lax.axis_index("dp")
        core, chip = index % 2, index // 2
        self.place = jnp.where(chip % 2 == 0, chip // 2, self.chips - 1 - chip // 2)
        rows = grads.shape[0] // size
        blocks = grads.reshape(self.chips, 2, rows, grads.shape[1])
        away = lax.dynamic_index_in_dim(blocks, 1 - core, 1, keepdims=False)
        mine = lax.dynamic_index_in_dim(blocks, core, 1, keepdims=False)
        swap = [(2 * at + c, 2 * at + 1 - c) for at in range(self.chips) for c in range(2)]
        arrived = lax.ppermute(away, "dp", swap)
        both = mine.astype(jnp.float32) + arrived.astype(jnp.float32)
        self.both = both.astype(self.low)
        self.hops = 0
        self.moving = None

    def own(self, offset):
        at = (self.place - self.step * offset + 2 * self.chips) % self.chips
        block = lax.dynamic_index_in_dim(self.both, chip_at(at, self.chips), 0, keepdims=False)
        return block.astype(jnp.float32)

    def hop(self):
        if self.hops == self.chips - 1:
            return
        if self.hops == 0:
            self.moving = self.own(1).astype(self.low)
        arrived = lax.ppermute(self.moving, "dp", ring_pairs(self.chips, self.step))
        total = arrived.astype(jnp.float32) + self.own(self.hops + 2)
        self.hops += 1
        self.moving = total if self.hops == self.chips - 1 else total.astype(self.low)

    def state(self):
        return self.both if self.moving is None else self.moving

    def set_state(self, value):
        if self.moving is None:
            self.both = value
        else:
            self.moving = value

    def finish(self):
        while self.hops < self.chips - 1:
            self.hop()
        return self.moving


def tie(values, *rings):
    values, states = lax.optimization_barrier((values, [ring.state() for ring in rings]))
    for ring, value in zip(rings, states):
        ring.set_state(value)
    return values


def hop_all(*rings):
    for ring in rings:
        ring.hop()


def solution(mesh):
    placed = (
        P(("dp", "tensor"), None),
        P("dp"),
        P("dp"),
        P("dp", "tensor"),
        P("dp", "tensor"),
        P("dp", "tensor"),
        P("dp", "tensor"),
        P("dp", "tensor"),
        P("tensor"),
        P("dp", "tensor"),
        P("dp"),
        P("dp", "tensor"),
        P("dp", "tensor"),
        P("dp", "tensor"),
        P(("dp", "tensor"), None),
    )
    return jax.shard_map(
        local,
        mesh=mesh,
        in_specs=placed,
        out_specs=(
            P(("dp", "tensor"), None),
            P(("dp", "tensor"), None),
            P("dp"),
            P("dp", "tensor"),
            P("dp", "tensor"),
            P("dp", "tensor"),
            P("dp", "tensor"),
            P("dp", "tensor"),
            P("tensor"),
            P("dp", "tensor"),
            P("dp"),
            P("dp", "tensor"),
            P("dp", "tensor"),
            P("dp", "tensor"),
        ),
        check_vma=False,
    )
```
